8 devices in a mesh: tp: 4 (over z, y, x), dp: 2 (over core).
Axes of the slice: x: 2, y: 2, z: 1, core: 2. Of those that a mesh axis runs over, the one named last changes fastest.
Arguments:
- x: bfloat16 [512, 2048], P('dp')
- lengths: int32 [512], P('dp')
- cache: bfloat16 [2, 512, 512, 576], P(None, 'dp')
- attn_norm: bfloat16 [2, 2048], replicated
- ffn_norm: bfloat16 [2, 2048], replicated
- wq: bfloat16 [2, 2048, 9216], P(None, None, 'tp')
- wo: bfloat16 [2, 8192, 2048], P(None, 'tp')
- w1: bfloat16 [2, 2048, 11264], P(None, None, ('dp', 'tp'))
- w3: bfloat16 [2, 2048, 11264], P(None, None, ('dp', 'tp'))
- w2: bfloat16 [2, 11264, 2048], P(None, ('dp', 'tp'))
Outputs:
- output: bfloat16 [512, 2048], P('dp')
All inputs are finite; a program needn't handle non-finite values.
Results may differ from the reference program's by a relative error of at most 0.02.
Values are sent between devices in bfloat16 or wider.
A program may use at most 1.5 GiB of HBM per device.

```python
import jax
import jax.numpy as jnp
from jax import lax

B = 512
S = 512
D = 2048
H = 16
F = 11264
LAYERS = 2
LAT = 512
ROPE = 64
KV = LAT + ROPE
EPS = 1e-6
SCALE = 192 ** -0.5


def setup_inputs(seed: int = 0) -> dict:
    ks = jax.random.split(jax.random.PRNGKey(seed), 10)

    def nrm(k, shape, std):
        return (jax.random.normal(k, shape, jnp.float32) * std).astype(jnp.bfloat16)

    def gain(k):
        return jax.random.uniform(k, (LAYERS, D), jnp.float32, 0.5, 1.5).astype(jnp.bfloat16)

    return {
        'x': nrm(ks[0], (B, D), 1.0),
        'lengths': jax.random.randint(ks[1], (B,), max(S // 8, 1), S + 1, jnp.int32),
        'cache': nrm(ks[2], (LAYERS, B, S, KV), 1.0),
        'attn_norm': gain(ks[3]),
        'ffn_norm': gain(ks[4]),
        'wq': nrm(ks[5], (LAYERS, D, H * KV), D ** -0.5),
        'wo': nrm(ks[6], (LAYERS, H * LAT, D), (H * LAT) ** -0.5 * S ** 0.5 / 8),
        'w1': nrm(ks[7], (LAYERS, D, F), D ** -0.5),
        'w3': nrm(ks[8], (LAYERS, D, F), D ** -0.5),
        'w2': nrm(ks[9], (LAYERS, F, D), 2.0 * F ** -0.5),
    }


def _rmsnorm(v, w):
    vf = v.astype(jnp.float32)
    r = lax.rsqrt(jnp.mean(vf * vf, axis=-1, keepdims=True) + EPS)
    return (vf * r * w.astype(jnp.float32)).astype(jnp.bfloat16)


def _attend(q, c, n):
    s = jnp.dot(q, c.T, preferred_element_type=jnp.float32) * SCALE
    s = jnp.where(jnp.arange(c.shape[0])[None, :] < n, s, -jnp.inf)
    p = jax.nn.softmax(s, axis=-1).astype(jnp.bfloat16)
    return jnp.dot(p, c[:, :LAT], preferred_element_type=jnp.float32).astype(jnp.bfloat16)


def _layer(x, lengths, c, an, fn, wq, wo, w1, w3, w2):
    nb = x.shape[0]
    h = _rmsnorm(x, an)
    q = jnp.dot(h, wq, preferred_element_type=jnp.float32).astype(jnp.bfloat16).reshape(nb, H, KV)
    o = lax.map(lambda t: _attend(*t), (q, c, lengths)).reshape(nb, H * LAT)
    x = x + jnp.dot(o, wo, preferred_element_type=jnp.float32).astype(jnp.bfloat16)
    g = _rmsnorm(x, fn)
    u = jnp.dot(g, w3, preferred_element_type=jnp.float32)
    v = jnp.dot(g, w1, preferred_element_type=jnp.float32)
    a = (jax.nn.silu(u) * v).astype(jnp.bfloat16)
    return x + jnp.dot(a, w2, preferred_element_type=jnp.float32).astype(jnp.bfloat16)


def reference(x, lengths, cache, attn_norm, ffn_norm, wq, wo, w1, w3, w2):
    def body(xc, lw):
        return _layer(xc, lengths, *lw), None
    out, _ = lax.scan(body, x, (cache, attn_norm, ffn_norm, wq, wo, w1, w3, w2))
    return out
```

```python
import functools

import jax
import jax.numpy as jnp
from jax import lax
from jax.experimental import pallas as pl
from jax.experimental.pallas import tpu as pltpu
from jax.sharding import PartitionSpec as P

LAT = 512
EPS = 1e-6
SCALE = 192 ** -0.5
MIB = 1024 * 1024


def _rmsnorm(v, w):
    vf = v.astype(jnp.float32)
    r = lax.rsqrt(jnp.mean(vf * vf, axis=-1, keepdims=True) + EPS)
    return (vf * r * w.astype(jnp.float32)).astype(jnp.bfloat16)


GROUP = 4
SLOTS = 3


def _attn_kernel(layer, rows, n_tp, lengths, q_ref, cache, o_ref, qf, of, buf, sem):
    hg, nb, cols = q_ref.shape
    s_len, kv = cache.shape[2], cache.shape[3]
    hpg = cols // kv
    nh = hg * hpg
    first = lax.axis_index('tp') * rows
    n_groups = rows // GROUP
    n_lane = qf.shape[0]

    def copies(g, slot):
        out = []
        for i in range(GROUP):
            out.append(pltpu.make_async_copy(
                cache.at[layer, first + g * GROUP + i], buf.at[slot, i], sem.at[slot, i]))
        return out

    for g in range(SLOTS - 1):
        for c in copies(g, g):
            c.start()

    for i in range(hg):
        for j in range(hpg // 2):
            pair = q_ref[i, :, 2 * kv * j:2 * kv * (j + 1)].astype(jnp.float32)
            other = pltpu.roll(pair, kv, 1)
            for k, v in ((2 * j, pair), (2 * j + 1, other)):
                h = i * hpg + k
                for n in range(n_lane):
                    qf[n, h * rows:(h + 1) * rows, :] = v[:, n * 128:(n + 1) * 128]

    def step(g, carry):
        slot = lax.rem(g, SLOTS)
        nxt = g + SLOTS - 1

        @pl.when(nxt < n_groups)
        def _():
            for c in copies(nxt, lax.rem(nxt, SLOTS)):
                c.start()

        for c in copies(g, slot):
            c.wait()
        for i in range(GROUP):
            b = g * GROUP + i
            q = jnp.concatenate([qf[n, pl.ds(b, nh, stride=rows), :] for n in range(n_lane)], axis=1)
            q = q[:, :kv].astype(jnp.bfloat16)
            c = buf[slot, i]
            s = lax.dot_general(q, c, (((1,), (1,)), ((), ())), preferred_element_type=jnp.float32) * SCALE
            pos = lax.broadcasted_iota(jnp.int32, s.shape, 1)
            s = jnp.where(pos < lengths[b], s, -jnp.inf)
            e = jnp.exp(s - jnp.max(s, axis=1, keepdims=True))
            p = (e / jnp.sum(e, axis=1, keepdims=True)).astype(jnp.bfloat16)
            o = jnp.dot(p, c[:, :LAT], preferred_element_type=jnp.float32)
            for n in range(LAT // 128):
                of[n, pl.ds(b, nh, stride=rows), :] = o[:, n * 128:(n + 1) * 128]
        return carry

    lax.fori_loop(0, n_groups, step, 0)
    for h in range(nh):
        for n in range(LAT // 128):
            k = (h % hpg) * LAT + n * 128
            o_ref[h // hpg, :, k:k + 128] = of[n, h * rows:(h + 1) * rows, :].astype(jnp.bfloat16)


def _attention(layer, q4, cache, lengths):
    hg, rows, cols = q4.shape
    s_len, kv = cache.shape[2:]
    nh = hg * cols // kv
    lanes = -(-kv // 128)
    return pl.pallas_call(
        functools.partial(_attn_kernel, layer, rows, hg),
        out_shape=jax.ShapeDtypeStruct((hg, rows, nh // hg * LAT), jnp.bfloat16),
        in_specs=[
            pl.BlockSpec(memory_space=pltpu.SMEM),
            pl.BlockSpec(memory_space=pltpu.VMEM),
            pl.BlockSpec(memory_space=pl.ANY),
        ],
        out_specs=pl.BlockSpec(memory_space=pltpu.VMEM),
        scratch_shapes=[
            pltpu.VMEM((lanes, nh * rows, 128), jnp.float32),
            pltpu.VMEM((LAT // 128, nh * rows, 128), jnp.float32),
            pltpu.VMEM((SLOTS, GROUP, s_len, kv), jnp.bfloat16),
            pltpu.SemaphoreType.DMA((SLOTS, GROUP)),
        ],
        compiler_params=pltpu.CompilerParams(vmem_limit_bytes=40 * MIB),
        cost_estimate=pl.CostEstimate(
            flops=4 * rows * nh * s_len * kv, bytes_accessed=rows * s_len * kv * 2, transcendentals=rows * nh * s_len),
        name=f'attention{layer}',
    )(lengths, q4, cache)


def solution(mesh):
    n_tp = mesh.shape['tp']

    def body(x, lengths, cache, attn_norm, ffn_norm, wq, wo, w1, w3, w2):
        nb, d = x.shape
        rows = nb // n_tp
        n_layers = cache.shape[0]
        me = lax.axis_index('tp')
        mine = lax.dynamic_slice_in_dim(lengths, me * rows, rows)
        xo = lax.dynamic_slice_in_dim(x, me * rows, rows)
        h = _rmsnorm(x, attn_norm[0])
        for l in range(n_layers):
            q = jnp.dot(h, wq[l], preferred_element_type=jnp.float32).astype(jnp.bfloat16)
            q4 = lax.all_to_all(q.reshape(n_tp, rows, -1), 'tp', 0, 0)
            o4 = _attention(l, q4, cache, mine)
            o = lax.all_to_all(o4, 'tp', 0, 0).reshape(nb, -1)
            attn = lax.psum_scatter(
                jnp.dot(o, wo[l], preferred_element_type=jnp.float32), 'tp', scatter_dimension=0, tiled=True)
            xo = xo + attn.astype(jnp.bfloat16)
            g = _rmsnorm(xo, ffn_norm[l])
            gg = lax.all_gather(g, ('dp', 'tp'), axis=0, tiled=True)
            u = jnp.dot(gg, w3[l], preferred_element_type=jnp.float32)
            v = jnp.dot(gg, w1[l], preferred_element_type=jnp.float32)
            a = (jax.nn.silu(u) * v).astype(jnp.bfloat16)
            yp = jnp.dot(a, w2[l], preferred_element_type=jnp.float32)
            y = lax.psum_scatter(yp, ('dp', 'tp'), scatter_dimension=0, tiled=True)
            xo = xo + y.astype(jnp.bfloat16)
            if l + 1 < n_layers:
                h = lax.all_gather(_rmsnorm(xo, attn_norm[l + 1]), 'tp', axis=0, tiled=True)
        return lax.all_gather(xo, 'tp', axis=0, tiled=True)

    in_specs = (
        P('dp', None),
        P('dp'),
        P(None, 'dp', None, None),
        P(None, None),
        P(None, None),
        P(None, None, 'tp'),
        P(None, 'tp', None),
        P(None, None, ('dp', 'tp')),
        P(None, None, ('dp', 'tp')),
        P(None, ('dp', 'tp'), None),
    )
    return jax.shard_map(body, mesh=mesh, in_specs=in_specs, out_specs=P('dp', None), check_vma=False)
```

```python
import functools

import jax
import jax.numpy as jnp
from jax import lax
from jax.experimental import pallas as pl
from jax.experimental.pallas import tpu as pltpu
from jax.sharding import PartitionSpec as P

LAT = 512
EPS = 1e-6
SCALE = 192 ** -0.5
MIB = 1024 * 1024


def _rmsnorm(v, w):
    vf = v.astype(jnp.float32)
    r = lax.rsqrt(jnp.mean(vf * vf, axis=-1, keepdims=True) + EPS)
    return (vf * r * w.astype(jnp.float32)).astype(jnp.bfloat16)


GROUP = 4
SLOTS = 3


def _attn_kernel(layer, rows, n_tp, lengths, q_ref, cache, o_ref, qf, of, buf, sem):
    hg, nb, cols = q_ref.shape
    kv = cache.shape[2]
    hpg = cols // kv
    nh = hg * hpg
    first = lax.axis_index('tp') * rows
    n_groups = rows // GROUP
    n_lane = qf.shape[0]

    def copies(g, slot):
        out = []
        for i in range(GROUP):
            out.append(pltpu.make_async_copy(
                cache.at[layer, first + g * GROUP + i], buf.at[slot, i], sem.at[slot, i]))
        return out

    for g in range(SLOTS - 1):
        for c in copies(g, g):
            c.start()

    for i in range(hg):
        for j in range(hpg // 2):
            pair = q_ref[i, :, 2 * kv * j:2 * kv * (j + 1)].astype(jnp.float32)
            other = pltpu.roll(pair, kv, 1)
            for k, v in ((2 * j, pair), (2 * j + 1, other)):
                h = i * hpg + k
                for n in range(n_lane):
                    qf[n, h * rows:(h + 1) * rows, :] = v[:, n * 128:(n + 1) * 128]

    def step(g, carry):
        slot = lax.rem(g, SLOTS)
        nxt = g + SLOTS - 1

        @pl.when(nxt < n_groups)
        def _():
            for c in copies(nxt, lax.rem(nxt, SLOTS)):
                c.start()

        for c in copies(g, slot):
            c.wait()
        for i in range(GROUP):
            b = g * GROUP + i
            q = jnp.concatenate([qf[n, pl.ds(b, nh, stride=rows), :] for n in range(n_lane)], axis=1)
            q = q[:, :kv].astype(jnp.bfloat16)
            c = buf[slot, i]
            s = jnp.dot(q, c, preferred_element_type=jnp.float32) * SCALE
            pos = lax.broadcasted_iota(jnp.int32, s.shape, 1)
            s = jnp.where(pos < lengths[b], s, -jnp.inf)
            e = jnp.exp(s - jnp.max(s, axis=1, keepdims=True))
            p = (e / jnp.sum(e, axis=1, keepdims=True)).astype(jnp.bfloat16)
            o = lax.dot_general(p, c[:LAT], (((1,), (1,)), ((), ())), preferred_element_type=jnp.float32)
            for n in range(LAT // 128):
                of[n, pl.ds(b, nh, stride=rows), :] = o[:, n * 128:(n + 1) * 128]
        return carry

    lax.fori_loop(0, n_groups, step, 0)
    for h in range(nh):
        for n in range(LAT // 128):
            k = (h % hpg) * LAT + n * 128
            o_ref[h // hpg, :, k:k + 128] = of[n, h * rows:(h + 1) * rows, :].astype(jnp.bfloat16)


def _attention(layer, q4, cache, lengths):
    hg, rows, cols = q4.shape
    kv, s_len = cache.shape[2:]
    nh = hg * cols // kv
    lanes = -(-kv // 128)
    return pl.pallas_call(
        functools.partial(_attn_kernel, layer, rows, hg),
        out_shape=jax.ShapeDtypeStruct((hg, rows, nh // hg * LAT), jnp.bfloat16),
        in_specs=[
            pl.BlockSpec(memory_space=pltpu.SMEM),
            pl.BlockSpec(memory_space=pltpu.VMEM),
            pl.BlockSpec(memory_space=pl.ANY),
        ],
        out_specs=pl.BlockSpec(memory_space=pltpu.VMEM),
        scratch_shapes=[
            pltpu.VMEM((lanes, nh * rows, 128), jnp.float32),
            pltpu.VMEM((LAT // 128, nh * rows, 128), jnp.float32),
            pltpu.VMEM((SLOTS, GROUP, kv, s_len), jnp.bfloat16),
            pltpu.SemaphoreType.DMA((SLOTS, GROUP)),
        ],
        compiler_params=pltpu.CompilerParams(vmem_limit_bytes=40 * MIB),
        cost_estimate=pl.CostEstimate(
            flops=4 * rows * nh * s_len * kv, bytes_accessed=rows * s_len * kv * 2, transcendentals=rows * nh * s_len),
        name=f'attention{layer}',
    )(lengths, q4, cache)


def solution(mesh):
    n_tp = mesh.shape['tp']

    def body(x, lengths, cache, attn_norm, ffn_norm, wq, wo, w1, w3, w2):
        nb, d = x.shape
        rows = nb // n_tp
        n_layers = cache.shape[0]
        cache = jnp.swapaxes(cache, 2, 3)
        me = lax.axis_index('tp')
        mine = lax.dynamic_slice_in_dim(lengths, me * rows, rows)
        xo = lax.dynamic_slice_in_dim(x, me * rows, rows)
        h = _rmsnorm(x, attn_norm[0])
        for l in range(n_layers):
            q = jnp.dot(h, wq[l], preferred_element_type=jnp.float32).astype(jnp.bfloat16)
            q4 = lax.all_to_all(q.reshape(n_tp, rows, -1), 'tp', 0, 0)
            o4 = _attention(l, q4, cache, mine)
            o = lax.all_to_all(o4, 'tp', 0, 0).reshape(nb, -1)
            attn = lax.psum_scatter(
                jnp.dot(o, wo[l], preferred_element_type=jnp.float32), 'tp', scatter_dimension=0, tiled=True)
            xo = xo + attn.astype(jnp.bfloat16)
            g = _rmsnorm(xo, ffn_norm[l])
            gg = lax.all_gather(g, ('dp', 'tp'), axis=0, tiled=True)
            u = jnp.dot(gg, w3[l], preferred_element_type=jnp.float32)
            v = jnp.dot(gg, w1[l], preferred_element_type=jnp.float32)
            a = (jax.nn.silu(u) * v).astype(jnp.bfloat16)
            yp = jnp.dot(a, w2[l], preferred_element_type=jnp.float32)
            y = lax.psum_scatter(yp, ('dp', 'tp'), scatter_dimension=0, tiled=True)
            xo = xo + y.astype(jnp.bfloat16)
            if l + 1 < n_layers:
                h = lax.all_gather(_rmsnorm(xo, attn_norm[l + 1]), 'tp', axis=0, tiled=True)
        return lax.all_gather(xo, 'tp', axis=0, tiled=True)

    in_specs = (
        P('dp', None),
        P('dp'),
        P(None, 'dp', None, None),
        P(None, None),
        P(None, None),
        P(None, None, 'tp'),
        P(None, 'tp', None),
        P(None, None, ('dp', 'tp')),
        P(None, None, ('dp', 'tp')),
        P(None, ('dp', 'tp'), None),
    )
    return jax.shard_map(body, mesh=mesh, in_specs=in_specs, out_specs=P('dp', None), check_vma=False)
```

```python
import functools

import jax
import jax.numpy as jnp
from jax import lax
from jax.experimental import pallas as pl
from jax.experimental.pallas import tpu as pltpu
from jax.sharding import PartitionSpec as P

LAT = 512
EPS = 1e-6
SCALE = 192 ** -0.5
MIB = 1024 * 1024
MESH = pl.DeviceIdType.MESH
BF, F32 = jnp.bfloat16, jnp.float32


def _rmsnorm(v, w):
    vf = v.astype(F32)
    r = lax.rsqrt(jnp.mean(vf * vf, axis=-1, keepdims=True) + EPS)
    return (vf * r * w.astype(F32)).astype(BF)


GROUP = 8
SLOTS = 3


def _attn_kernel(layer, rows, lengths, q_ref, cache, o_ref, qf, of, buf, sem):
    hg, nb, cols = q_ref.shape
    kv = cache.shape[2]
    hpg = cols // kv
    nh = hg * hpg
    first = lax.axis_index('tp') * rows
    n_groups = rows // GROUP
    n_lane = qf.shape[0]

    def copies(g, slot):
        return [pltpu.make_async_copy(cache.at[layer, first + g * GROUP + i], buf.at[slot, i], sem.at[slot, i])
                for i in range(GROUP)]

    for g in range(SLOTS - 1):
        for c in copies(g, g):
            c.start()

    for i in range(hg):
        for j in range(hpg // 2):
            pair = q_ref[i, :, 2 * kv * j:2 * kv * (j + 1)].astype(F32)
            other = pltpu.roll(pair, kv, 1)
            for k, v in ((2 * j, pair), (2 * j + 1, other)):
                h = i * hpg + k
                for n in range(n_lane):
                    qf[n, h * rows:(h + 1) * rows, :] = v[:, n * 128:(n + 1) * 128]

    def step(g, carry):
        slot = lax.rem(g, SLOTS)
        nxt = g + SLOTS - 1

        @pl.when(nxt < n_groups)
        def _():
            for c in copies(nxt, lax.rem(nxt, SLOTS)):
                c.start()

        for c in copies(g, slot):
            c.wait()
        ss, ps = [], []
        for i in range(GROUP):
            b = g * GROUP + i
            q = jnp.concatenate([qf[n, pl.ds(b, nh, stride=rows), :] for n in range(n_lane)], axis=1)
            q = q[:, :kv].astype(BF)
            ss.append(jnp.dot(q, buf[slot, i], preferred_element_type=F32) * SCALE)
        for i in range(GROUP):
            s = ss[i]
            pos = lax.broadcasted_iota(jnp.int32, s.shape, 1)
            s = jnp.where(pos < lengths[g * GROUP + i], s, -jnp.inf)
            e = jnp.exp(s - jnp.max(s, axis=1, keepdims=True))
            ps.append((e / jnp.sum(e, axis=1, keepdims=True)).astype(BF))
        for i in range(GROUP):
            o = lax.dot_general(ps[i], buf[slot, i, :LAT], (((1,), (1,)), ((), ())), preferred_element_type=F32)
            for n in range(LAT // 128):
                of[n, pl.ds(g * GROUP + i, nh, stride=rows), :] = o[:, n * 128:(n + 1) * 128]
        return carry

    lax.fori_loop(0, n_groups, step, 0)
    for h in range(nh):
        for n in range(LAT // 128):
            k = (h % hpg) * LAT + n * 128
            o_ref[h // hpg, :, k:k + 128] = of[n, h * rows:(h + 1) * rows, :].astype(BF)


def _attention(layer, q4, cache, lengths):
    hg, rows, cols = q4.shape
    kv, s_len = cache.shape[2:]
    nh = hg * cols // kv
    lanes = -(-kv // 128)
    return pl.pallas_call(
        functools.partial(_attn_kernel, layer, rows),
        out_shape=jax.ShapeDtypeStruct((hg, rows, nh // hg * LAT), BF),
        in_specs=[
            pl.BlockSpec(memory_space=pltpu.SMEM),
            pl.BlockSpec(memory_space=pltpu.VMEM),
            pl.BlockSpec(memory_space=pl.ANY),
        ],
        out_specs=pl.BlockSpec(memory_space=pltpu.VMEM),
        scratch_shapes=[
            pltpu.VMEM((lanes, nh * rows, 128), F32),
            pltpu.VMEM((LAT // 128, nh * rows, 128), F32),
            pltpu.VMEM((SLOTS, GROUP, kv, s_len), BF),
            pltpu.SemaphoreType.DMA((SLOTS, GROUP)),
        ],
        compiler_params=pltpu.CompilerParams(vmem_limit_bytes=50 * MIB),
        cost_estimate=pl.CostEstimate(
            flops=4 * rows * nh * s_len * kv, bytes_accessed=rows * s_len * kv * 2, transcendentals=rows * nh * s_len),
        name=f'attention{layer}',
    )(lengths, q4, cache)


def _remote(src, dst, ssem, rsem, dev):
    return pltpu.make_async_remote_copy(
        src_ref=src, dst_ref=dst, send_sem=ssem, recv_sem=rsem,
        device_id={'tp': dev[0], 'dp': dev[1]}, device_id_type=MESH)


def _places():
    tp, dp = lax.axis_index('tp'), lax.axis_index('dp')
    x, y = lax.rem(tp, 2), tp // 2
    chips = (tp, y * 2 + 1 - x, (1 - y) * 2 + x, (1 - y) * 2 + 1 - x)
    return chips, dp


def _barrier(devs):
    sem = pltpu.get_barrier_semaphore()
    for t, d in devs:
        pl.semaphore_signal(sem, inc=1, device_id={'tp': t, 'dp': d}, device_id_type=MESH)
    pl.semaphore_wait(sem, len(devs))


HOPS = (None, 1, 2)


class _Gather:
    def __init__(self, blk, to, chips, dp, ssem, rsem):
        self.blk, self.to, self.chips, self.dp, self.ssem, self.rsem = blk, to, chips, dp, ssem, rsem
        half = blk(0).shape[-1] // 2
        self.cut = [pl.ds(0, half), pl.ds(half, half)]

    def _hop(self, r, hop, half, k):
        return _remote(self.blk(r).at[:, self.cut[half]], self.to(r, hop).at[:, self.cut[half]],
                       self.ssem.at[k], self.rsem.at[k], (self.chips[hop], self.dp))

    def direct(self, hop, half):
        return self._hop(0, hop, half, (hop - 1) * 2 + half)

    def relay(self, hop):
        return self._hop(3 - hop, hop, 0 if hop == 2 else 1, 4 + hop - 1)

    def start(self):
        for hop, half in ((1, 0), (2, 1), (1, 1), (2, 0)):
            self.direct(hop, half).start()

    def near(self):
        self.direct(1, 0).wait_recv()
        self.relay(2).start()
        self.direct(2, 1).wait_recv()
        self.relay(1).start()

    def near_rest(self, hop):
        self.direct(hop, 1 if hop == 1 else 0).wait_recv()

    def far(self):
        self.relay(1).wait_recv()
        self.relay(2).wait_recv()

    def finish(self):
        for hop in (1, 2):
            self.direct(hop, 0).wait_send()
            self.direct(hop, 1).wait_send()
            self.relay(hop).wait_send()


CW = 256


def _scatter(sent, kept, s1, r1, kp, s2, r2, sem1s, sem1r, sem2s, sem2r, chips, dp, after=None):
    n = s1.shape[1]
    rows = s2.shape[2]

    def one(p, j):
        return _remote(s1.at[p, j], r1.at[p, j], sem1s.at[p, j], sem1r.at[p, j], (chips[1 + p], dp))

    def two(p, j):
        return _remote(s2.at[p, j], r2.at[p, j], sem2s.at[p, j], sem2r.at[p, j], (chips[2 - p], dp))

    def send(j, c):
        sent(j)
        for p in range(2):
            one(p, j).start()
        return c

    def forward(j, c):
        if after is None:
            kept(j)
        for p in range(2):
            one(p, j).wait_recv()
            s2[p, j] = kp[p, j, rows:] + r1[p, j, rows:]
            two(p, j).start()
        return c

    lax.fori_loop(0, n, send, 0)
    if after is not None:
        after()
    lax.fori_loop(0, n, forward, 0)

    def total(p, j):
        two(p, j).wait_recv()
        return kp[p, j, :rows] + r1[p, j, :rows] + r2[p, j]

    def finish():
        def fin(j, c):
            for p in range(2):
                one(p, j).wait_send()
                two(p, j).wait_send()
            return c
        lax.fori_loop(0, n, fin, 0)

    return total, finish


def _first_kernel(x_ref, norm, wq_h, q_out, wq, qs, wsem, ssem, rsem):
    chips, dp = _places()
    w = pltpu.make_async_copy(wq_h.at[0], wq, wsem)
    w.start()
    _barrier([(chips[r], dp) for r in (1, 2, 3)])
    w.wait()
    _q_blocks(lambda r: _rmsnorm(x_ref[chips[r]], norm[0:1, :]), (3, 1, 2, 0), chips, dp, wq, qs, q_out, ssem, rsem)


def _q_blocks(h_of, order, chips, dp, wq, qs, q_out, ssem, rsem):
    def send(r):
        return _remote(qs.at[r], q_out.at[chips[0]], ssem.at[r], rsem.at[r], (chips[r], dp))

    n = wq.shape[1] // CW
    for r in order:
        h = h_of(r)
        dst = qs.at[r] if r else q_out.at[chips[0]]

        def tile(t, c):
            cols = pl.ds(pl.multiple_of(t * CW, CW), CW)
            dst[:, cols] = jnp.dot(h, wq[:, cols], preferred_element_type=F32).astype(BF)
            return c

        lax.fori_loop(0, n, tile, 0)
        if r:
            send(r).start()
    for r in (1, 2, 3):
        send(r).wait_recv()
    for r in (1, 2, 3):
        send(r).wait_send()


def _layer_kernel(layer, last, o_ref, x_ref, fnorm, anorm, wo_h, w1_h, w3_h, w2_h, wq_h, *refs):
    if last:
        out, *refs = refs
    else:
        q_out, x_out, *refs = refs
    (wo, w1, w3, w2, wsem, ob, osem_s, osem_r,
     as1, ar1, akp, as2, ar2, asem, xs,
     g, gsem_s, gsem_r, dsem_s, dsem_r, act,
     lp, ds, dr, dds_s, dds_r, fs1, fr1, fkp, fs2, fr2, fsem, *refs) = refs
    chips, dp = _places()
    sib = (chips[0], 1 - dp)
    rows, d = x_ref.shape
    half = d // 2
    nch = half // CW

    srcs = [(wo_h, wo), (w3_h, w3), (w1_h, w1), (w2_h, w2)]
    if not last:
        wq, h_all, qs, hsem_s, hsem_r, qsem_s, qsem_r = refs
        srcs.append((wq_h, wq))
    else:
        hsem_s, hsem_r = refs
    loads = [pltpu.make_async_copy(s.at[layer + (s is wq_h)], v, wsem.at[i]) for i, (s, v) in enumerate(srcs)]
    for c in loads:
        c.start()
    _barrier([(chips[r], dp) for r in (1, 2, 3)] + [sib])

    def osend(r):
        return _remote(o_ref.at[chips[r]], ob.at[r], osem_s.at[r], osem_r.at[r], (chips[r], dp))

    for r in (3, 1, 2):
        osend(r).start()
    ob[0] = o_ref[chips[0]]
    for r in (1, 2, 3):
        osend(r).wait_recv()
    loads[0].wait()

    def cols(p, j):
        return pl.ds(pl.multiple_of(p * half + j * CW, CW), CW)

    def o_dot(a, b, p, j):
        lhs = jnp.concatenate([ob[a], ob[b]], axis=0)
        return jnp.dot(lhs, wo[:, cols(p, j)], preferred_element_type=F32)

    def sent(j):
        for p in range(2):
            as1[p, j] = o_dot(1 + p, 3, p, j)

    def kept(j):
        for p in range(2):
            akp[p, j] = o_dot(0, 2 - p, p, j)

    total, finish_a = _scatter(sent, kept, as1, ar1, akp, as2, ar2, asem.at[0], asem.at[1], asem.at[2], asem.at[3],
                               chips, dp)
    for p in range(2):
        for j in range(nch):
            c = slice(p * half + j * CW, p * half + (j + 1) * CW)
            xs[:, c] = x_ref[:, c] + total(p, j).astype(BF)

    g[0, 0] = _rmsnorm(xs[...], fnorm[layer:layer + 1, :])
    ag = _Gather(lambda r: g.at[r, 0], lambda r, hop: g.at[r ^ hop, 0], chips, dp, gsem_s, gsem_r)

    def cross(r):
        return _remote(g.at[r, 0], g.at[r, 1], dsem_s.at[r], dsem_r.at[r], sib)

    ag.start()
    cross(0).start()
    ag.near()
    ag.near_rest(1)
    cross(1).start()
    ag.near_rest(2)
    cross(2).start()
    for c in loads[1:3]:
        c.wait()
    for r in range(3):
        cross(r).wait_recv()

    f = w1.shape[1]
    full = f // CW

    def up(lo, hi, t0, t1, tail):
        m = (hi - lo) * 2 * rows

        def gate(u, v, cc, w):
            act[lo:hi, :, :, cc] = (jax.nn.silu(u) * v).astype(BF).reshape(hi - lo, 2, rows, w)

        def tile(t, c):
            cc = pl.ds(pl.multiple_of(t * CW, CW), CW)
            gg = g[lo:hi].reshape(m, d)
            u = jnp.dot(gg, w3[:, cc], preferred_element_type=F32)
            v = jnp.dot(gg, w1[:, cc], preferred_element_type=F32)
            gate(u, v, cc, CW)
            return c

        lax.fori_loop(t0, t1, tile, 0)
        if tail:
            gg = g[lo:hi].reshape(m, d)
            w = f - full * CW
            ww = jnp.concatenate([w3[:, full * CW:], w1[:, full * CW:]], axis=1)
            uv = jnp.dot(gg, ww, preferred_element_type=F32)
            gate(uv[:, :w], uv[:, w:], slice(full * CW, f), w)

    up(0, 3, 0, 3, False)
    ag.far()
    cross(3).start()
    up(0, 3, 3, full, True)
    cross(3).wait_recv()
    up(3, 4, 0, full, True)
    loads[3].wait()

    def dsend(k, p, j):
        return _remote(ds.at[k, p, j], dr.at[k, p, j], dds_s.at[k, p, j], dds_r.at[k, p, j], sib)

    def f_dot(k, j, c):
        for p in range(2):
            a, b = ((1 + p, 3), (0, 2 - p))[k]
            lhs = jnp.concatenate([act[a, 1], act[b, 1], act[a, 0], act[b, 0]], axis=0)
            res = jnp.dot(lhs, w2[:, cols(p, j)], preferred_element_type=F32)
            ds[k, p, j] = res[:2 * rows]
            dsend(k, p, j).start()
            lp[k, p, j] = res[2 * rows:]
        return c

    lax.fori_loop(0, nch, functools.partial(f_dot, 0), 0)

    def joined(k, dst, j):
        for p in range(2):
            dsend(k, p, j).wait_recv()
            dst[p, j] = lp[k, p, j] + dr[k, p, j]

    def after():
        lax.fori_loop(0, nch, functools.partial(f_dot, 1), 0)

        def join(j, c):
            joined(1, fkp, j)
            return c
        lax.fori_loop(0, nch, join, 0)

    total, finish_f = _scatter(functools.partial(joined, 0, fs1), None, fs1, fr1, fkp, fs2, fr2,
                               fsem.at[0], fsem.at[1], fsem.at[2], fsem.at[3], chips, dp, after)
    for p in range(2):
        for j in range(nch):
            c = slice(p * half + j * CW, p * half + (j + 1) * CW)
            xs[:, c] = xs[:, c] + total(p, j).astype(BF)

    if last:
        me = chips[0]
        out[me] = xs[...]
        hg = _Gather(lambda r: out.at[chips[r]], lambda r, hop: out.at[chips[r]], chips, dp, hsem_s, hsem_r)
        hg.start()
        hg.near()
        hg.near_rest(1)
        hg.near_rest(2)
        hg.far()
    else:
        x_out[...] = xs[...]
        h_all[0] = _rmsnorm(xs[...], anorm[layer + 1:layer + 2, :])
        hg = _Gather(lambda r: h_all.at[r], lambda r, hop: h_all.at[r ^ hop], chips, dp, hsem_s, hsem_r)
        hg.start()
        loads[4].wait()

        def h_of(r):
            if r == 1:
                hg.near()
            if r == 3:
                hg.far()
            elif r:
                hg.near_rest(r)
            return h_all[r]

        _q_blocks(h_of, (0, 1, 2, 3), chips, dp, wq, qs, q_out, qsem_s, qsem_r)

    for r in (1, 2, 3):
        osend(r).wait_send()
    finish_a()
    ag.finish()
    for r in range(4):
        cross(r).wait_send()

    def fin(j, c):
        for k in range(2):
            for p in range(2):
                dsend(k, p, j).wait_send()
        return c
    lax.fori_loop(0, nch, fin, 0)
    finish_f()
    hg.finish()


VM = pl.BlockSpec(memory_space=pltpu.VMEM)
HB = pl.BlockSpec(memory_space=pl.ANY)
DMA = pltpu.SemaphoreType.DMA


def _first(x, norm, wq):
    nb, d = x.shape
    rows = nb // 4
    qc = wq.shape[2]
    return pl.pallas_call(
        _first_kernel,
        out_shape=jax.ShapeDtypeStruct((4, rows, qc), BF),
        in_specs=[VM, VM, HB],
        out_specs=VM,
        scratch_shapes=[pltpu.VMEM((d, qc), BF), pltpu.VMEM((4, rows, qc), BF), DMA, DMA((4,)), DMA((4,))],
        compiler_params=pltpu.CompilerParams(collective_id=0, has_side_effects=True, vmem_limit_bytes=50 * MIB),
        name='first',
    )(x.reshape(4, rows, d), norm, wq)


def _layer(layer, last, o4, xo, fnorm, anorm, wo, w1, w3, w2, wq):
    rows, d = xo.shape
    ko = o4.shape[2]
    f = w1.shape[2]
    qc = wq.shape[2]
    nch = d // 2 // CW
    pair = lambda r: pltpu.VMEM((2, nch, r, CW), F32)
    quad = pltpu.VMEM((2, 2, nch, 2 * rows, CW), F32)
    scratch = [
        pltpu.VMEM((ko, d), BF), pltpu.VMEM((d, f), BF), pltpu.VMEM((d, f), BF), pltpu.VMEM((f, d), BF), DMA((5,)),
        pltpu.VMEM((4, rows, ko), BF), DMA((4,)), DMA((4,)),
        pair(2 * rows), pair(2 * rows), pair(2 * rows), pair(rows), pair(rows), DMA((4, 2, nch)),
        pltpu.VMEM((rows, d), BF),
        pltpu.VMEM((4, 2, rows, d), BF), DMA((6,)), DMA((6,)), DMA((4,)), DMA((4,)),
        pltpu.VMEM((4, 2, rows, f), BF),
        quad, quad, quad, DMA((2, 2, nch)), DMA((2, 2, nch)),
        pair(2 * rows), pair(2 * rows), pair(2 * rows), pair(rows), pair(rows), DMA((4, 2, nch)),
    ]
    if last:
        out_shape = jax.ShapeDtypeStruct((4, rows, d), BF)
        out_specs = VM
        scratch += [DMA((6,)), DMA((6,))]
    else:
        out_shape = (jax.ShapeDtypeStruct((4, rows, qc), BF), jax.ShapeDtypeStruct((rows, d), BF))
        out_specs = (VM, VM)
        scratch += [pltpu.VMEM((d, qc), BF), pltpu.VMEM((4, rows, d), BF), pltpu.VMEM((4, rows, qc), BF),
                    DMA((6,)), DMA((6,)), DMA((4,)), DMA((4,))]
    return pl.pallas_call(
        functools.partial(_layer_kernel, layer, last),
        out_shape=out_shape,
        in_specs=[VM, VM, VM, VM, HB, HB, HB, HB, HB],
        out_specs=out_specs,
        scratch_shapes=scratch,
        compiler_params=pltpu.CompilerParams(
            collective_id=1 + layer, has_side_effects=True, vmem_limit_bytes=63 * MIB),
        name=f'layer{layer}',
    )(o4, xo, fnorm, anorm, wo, w1, w3, w2, wq)


def solution(mesh):
    n_tp = mesh.shape['tp']

    def body(x, lengths, cache, attn_norm, ffn_norm, wq, wo, w1, w3, w2):
        nb, d = x.shape
        rows = nb // n_tp
        n_layers = cache.shape[0]
        cache = jnp.swapaxes(cache, 2, 3)
        me = lax.axis_index('tp')
        mine = lax.dynamic_slice_in_dim(lengths, me * rows, rows)
        xo = lax.dynamic_slice_in_dim(x, me * rows, rows)
        q4 = _first(x, attn_norm, wq)
        for l in range(n_layers):
            last = l + 1 == n_layers
            o4 = _attention(l, q4, cache, mine)
            res = _layer(l, last, o4, xo, ffn_norm, attn_norm, wo, w1, w3, w2, wq)
            if not last:
                q4, xo = res
        return res.reshape(nb, d)

    in_specs = (
        P('dp', None),
        P('dp'),
        P(None, 'dp', None, None),
        P(None, None),
        P(None, None),
        P(None, None, 'tp'),
        P(None, 'tp', None),
        P(None, None, ('dp', 'tp')),
        P(None, None, ('dp', 'tp')),
        P(None, ('dp', 'tp'), None),
    )
    return jax.shard_map(body, mesh=mesh, in_specs=in_specs, out_specs=P('dp', None), check_vma=False)
```
